32 devices in a mesh: dp: 4 (over y, x), vocab: 8 (over z, core).
Axes of the slice: x: 2, y: 2, z: 4, core: 2. Of those that a mesh axis runs over, the one named last changes fastest.
Arguments:
- hidden: bfloat16 [1024, 8192], P('dp'), may hold values from -14 to 14
- weight: bfloat16 [8192, 8192], P('dp', 'vocab'), may hold values from -1 to 1, as said below
- targets: int32 [1024], P('dp'), may hold values from 0 to 8191
- cotangent: float32 [1024], P('dp'), may hold values from 1 to 8
Outputs:
- loss: float32 [1024], P('dp')
- grad_hidden: bfloat16 [1024, 8192], P('vocab', 'dp')
- grad_weight: bfloat16 [8192, 8192], P('dp', 'vocab')
The draws below stay inside these ranges and needn't reach their ends.
Inputs may be any that keep to these rules, and one draw needn't show every extreme that they name: `weight`: entries drawn with standard deviation 4 / sqrt(8192).
All inputs are finite; a program needn't handle non-finite values.
Results may differ from the reference program's by a relative error of at most 0.0047.
Values may be sent and summed in bfloat16 or wider, within the bound.
A program may use at most 128 MiB of HBM per device.

```python
import math
import jax
import jax.numpy as jnp
from jax import lax

D = 8192
VOCAB = 8192
TOKENS = 1024


def joint_draw(key):
    weight_key = jax.random.fold_in(key, 11)
    hidden_key = jax.random.fold_in(key, 12)
    weight = jnp.clip(jnp.clip(jax.random.normal(weight_key, (D, VOCAB), jnp.float32), -6.0, 6.0) * (4.0 / D ** 0.5), -1.0, 1.0)
    hidden = jnp.clip(jax.random.normal(hidden_key, (TOKENS, D), jnp.float32), -6.0, 6.0)
    return (weight, hidden)


def draw_weight(key, part):
    weight, hidden = joint_draw(key)
    return weight.astype(jnp.bfloat16)


def draw_hidden(key, part):
    weight, hidden = joint_draw(key)
    return hidden.astype(jnp.bfloat16)


def set_ends(result, key, smallest, top_value):
    longest = result.shape.index(max(result.shape))
    spots = []
    for shift in (0, 1):
        where = [jax.random.randint(jax.random.fold_in(key, axis), (), 0, length) for axis, length in enumerate(result.shape)]
        where[longest] = (where[longest] + shift) % result.shape[longest]
        spots.append(tuple(where))
    return result.at[spots[0]].set(smallest).at[spots[1]].set(top_value)


def shard_levels(own_key, dims, split, smallest, top_value):
    def one(position, shards_of):
        steps = jax.random.uniform(jax.random.fold_in(jax.random.fold_in(own_key, 6), position), (shards_of,), jnp.float32, smallest / len(split), top_value / len(split))
        return jnp.repeat(jnp.exp(steps), dims[position] // shards_of).reshape((-1,) + (1,) * (len(dims) - position - 1))

    gain = one(*split[0])
    for cut in split[1:]:
        gain = gain * one(*cut)
    return gain


def setup_inputs(seed: int = 0) -> dict:
    key_list = jax.random.split(jax.random.key(seed), 5)
    return {
        "hidden": draw_hidden(jax.random.fold_in(key_list[4], 71), 0),
        "weight": draw_weight(jax.random.fold_in(key_list[4], 71), 0),
        "targets": set_ends(jax.random.randint(key_list[2], (TOKENS,), 0, VOCAB), jax.random.fold_in(key_list[2], 1), 0, VOCAB - 1).astype(jnp.int32),
        "cotangent": jnp.clip(jnp.exp(math.log(8.0) - 2.0794415 * jax.random.uniform(key_list[3], (TOKENS,), jnp.float32) ** shard_levels(key_list[3], (TOKENS,), ((0, 4),), -0.2, 0.2)), 1.0, 8.0),
    }


def reference(hidden, weight, targets, cotangent):
    logits = jnp.dot(hidden, weight, preferred_element_type=jnp.float32)
    row_max = jnp.max(logits, axis=1, keepdims=True)
    shifted = jnp.exp(logits - row_max)
    sum_exp = jnp.sum(shifted, axis=1, keepdims=True)
    columns = jnp.arange(VOCAB, dtype=jnp.int32)
    onehot = (targets.astype(jnp.int32)[:, None] == columns[None, :]).astype(jnp.float32)
    picked = jnp.sum(logits * onehot, axis=1)
    loss = row_max[:, 0] + jnp.log(sum_exp[:, 0]) - picked
    grad_logits = (cotangent[:, None] * (shifted / sum_exp - onehot)).astype(jnp.bfloat16)
    grad_hidden = lax.dot_general(grad_logits, weight, (((1,), (1,)), ((), ())), preferred_element_type=jnp.float32).astype(jnp.bfloat16)
    grad_weight = lax.dot_general(hidden, grad_logits, (((0,), (0,)), ((), ())), preferred_element_type=jnp.float32).astype(jnp.bfloat16)
    return (loss, grad_hidden, grad_weight)
```

```python
import functools

import jax
import jax.numpy as jnp
from jax import lax
from jax.experimental import pallas as pl
from jax.experimental.pallas import tpu as pltpu
from jax.sharding import PartitionSpec as P

F32 = jnp.float32
BF16 = jnp.bfloat16
WIRE = jnp.int16
STEPS = 32000.0


def kernel(
    nd, nv, levels,
    h_ref, w_hbm, t_ref, c_ref,
    loss_ref, gh_ref, gw_ref,
    w, spread, logit, psend, precv, stats, grads, acc, sbuf, rbuf, gwbuf, tcol, ccol, col,
    part_f32, usend, urecv, ucol,
    w_sem, own_sem, gw_sem,
    hs_send, hs_recv, hf_send, hf_recv, p_send, p_recv, u_send, u_recv,
    st_send, st_recv, g_send, g_recv, r_send, r_recv,
):
    d, v = lax.axis_index("dp"), lax.axis_index("vocab")
    core = lax.rem(v, 2)
    mate = v + 1 - 2 * core
    depth, width = w.shape
    tokens = spread.shape[0]
    rows = tokens // nd
    half = rows // 2
    share = tokens // nv
    per = rows // share

    load_w = pltpu.make_async_copy(w_hbm, w, w_sem)
    load_w.start()
    own_rows = pl.ds(pl.multiple_of(d * rows, rows), rows)
    load_own = pltpu.make_async_copy(
        h_ref.at[:, pl.ds(pl.multiple_of(d * depth, depth), depth)], spread.at[own_rows], own_sem
    )
    load_own.start()

    barrier = pltpu.get_barrier_semaphore()
    for k in range(1, nd):
        pl.semaphore_signal(barrier, inc=1, device_id={"dp": lax.rem(d + k, nd)})
    for k in range(1, nv):
        pl.semaphore_signal(barrier, inc=1, device_id={"vocab": lax.rem(v + k, nv)})
    pl.semaphore_wait(barrier, nd + nv - 2)

    def remote(src, dst, send, recv, where):
        return pltpu.make_async_remote_copy(
            src_ref=src, dst_ref=dst, send_sem=send, recv_sem=recv, device_id=where
        )

    hidden_sends = []
    for k in range(1, nd):
        to = lax.rem(d + k, nd)
        copy = remote(
            h_ref.at[pl.ds(pl.multiple_of(core * half, half), half), pl.ds(pl.multiple_of(to * depth, depth), depth)],
            spread.at[pl.ds(pl.multiple_of(d * rows + core * half, half), half)],
            hs_send.at[k - 1], hs_recv.at[k - 1], {"dp": to},
        )
        copy.start()
        hidden_sends.append(copy)

    tcol[...] = jnp.broadcast_to(t_ref[...], (128, rows)).T
    ccol[...] = jnp.broadcast_to(c_ref[...], (128, rows)).T

    tile = min(256, width)
    code_rows = min(32, half)

    def project(first, count, store):
        def step(n, _):
            cols = pl.ds(pl.multiple_of(n * tile, tile), tile)
            store(cols, jnp.dot(
                spread[pl.ds(pl.multiple_of(first, count), count), :], w[:, cols],
                preferred_element_type=F32,
            ))
            return 0

        lax.fori_loop(0, width // tile, step, 0)

    load_w.wait()
    load_own.wait()

    def store_own(cols, value):
        logit[:, cols] = value

    project(d * rows, rows, store_own)

    forwards, partial_sends = [], []
    for k in range(1, nd):
        s = lax.rem(d + nd - k, nd)
        for turn in range(2):
            part = core if turn == 0 else 1 - core
            block = spread.at[pl.ds(pl.multiple_of(s * rows + part * half, half), half)]
            if turn == 0:
                remote(block, block, hs_send.at[k - 1], hs_recv.at[k - 1], {"dp": s}).wait_recv()
                copy = remote(block, block, hf_send.at[k - 1], hf_recv.at[k - 1], {"vocab": mate})
                copy.start()
                forwards.append(copy)
            else:
                remote(block, block, hf_send.at[k - 1], hf_recv.at[k - 1], {"vocab": mate}).wait_recv()
            there = pl.ds(pl.multiple_of(part * half, half), half)

            def store_part(cols, value):
                part_f32[:, cols] = value

            project(s * rows + part * half, half, store_part)

            def encode(i, _, k=k, part=part):
                at = pl.ds(pl.multiple_of(i * code_rows, code_rows), code_rows)
                x = part_f32[at, :]
                unit = jnp.maximum(jnp.max(jnp.abs(x), axis=1, keepdims=True), 1e-30) / STEPS
                there = pl.ds(pl.multiple_of(part * half + i * code_rows, code_rows), code_rows)
                psend[k - 1, there, :] = jnp.round(x / unit).astype(jnp.int32).astype(WIRE)
                col[at, :] = jnp.broadcast_to(unit, (code_rows, 128))
                return 0

            lax.fori_loop(0, half // code_rows, encode, 0)
            usend[k - 1, turn] = col[:half, :].T[:8, :]
            for copy in (
                remote(
                    psend.at[k - 1, there], precv.at[k - 1, there],
                    p_send.at[k - 1, turn], p_recv.at[k - 1, turn], {"dp": s},
                ),
                remote(
                    usend.at[k - 1, turn], urecv.at[k - 1, turn],
                    u_send.at[k - 1, turn], u_recv.at[k - 1, turn], {"dp": s},
                ),
            ):
                copy.start()
                partial_sends.append(copy)
    for copy in partial_sends:
        copy.wait_recv()
    for k in range(1, nd):
        for turn in range(2):
            part = core if turn == 0 else 1 - core
            there = pl.ds(pl.multiple_of(part * half, half), half)
            ucol[k - 1, there, :] = jnp.broadcast_to(urecv[k - 1, turn][0:1, :], (128, half)).T

    step_rows = min(32, rows)
    column = lax.broadcasted_iota(jnp.int32, (step_rows, width), 1) + v * width
    lane = lax.broadcasted_iota(jnp.int32, (step_rows, 128), 1)

    def measure(i, _):
        at = pl.ds(pl.multiple_of(i * step_rows, step_rows), step_rows)
        x = logit[at, :]
        for k in range(1, nd):
            x = x + precv[k - 1, at, :].astype(jnp.int32).astype(F32) * ucol[k - 1, at, :1]
        top = jnp.max(x, axis=1, keepdims=True)
        e = jnp.exp(x - top)
        total = jnp.sum(e, axis=1, keepdims=True)
        pick = jnp.sum(jnp.where(column == tcol[at, :1], x, 0.0), axis=1, keepdims=True)
        logit[at, :] = e
        col[at, :] = jnp.where(lane == 0, top, jnp.where(lane == 1, total, pick))
        return 0

    lax.fori_loop(0, rows // step_rows, measure, 0)
    stats[v] = col[...].T[:8, :]
    stat_sends = []
    for k in range(1, nv):
        copy = remote(
            stats.at[v], stats.at[v], st_send.at[k - 1], st_recv.at[k - 1],
            {"vocab": lax.rem(v + k, nv)},
        )
        copy.start()
        stat_sends.append(copy)
    own_top = stats[v][0:1, :]
    for copy in stat_sends:
        copy.wait_recv()
    top = stats[0][0:1, :]
    for u in range(1, nv):
        top = jnp.maximum(top, stats[u][0:1, :])
    total = jnp.zeros_like(top)
    pick = jnp.zeros_like(top)
    for u in range(nv):
        block = stats[u]
        total = total + block[1:2, :] * jnp.exp(block[0:1, :] - top)
        pick = pick + block[2:3, :]
    loss_ref[...] = top + jnp.log(total) - pick
    scale = c_ref[...] * jnp.exp(own_top - top) / total
    col[...] = jnp.broadcast_to(scale, (128, rows)).T

    def differentiate(i, _):
        at = pl.ds(pl.multiple_of(i * step_rows, step_rows), step_rows)
        onehot = jnp.where(column == tcol[at, :1], ccol[at, :1], 0.0)
        g = logit[at, :] * col[at, :1] - onehot
        grads[pl.ds(pl.multiple_of(d * rows + i * step_rows, step_rows), step_rows), :] = g.astype(BF16)
        return 0

    lax.fori_loop(0, rows // step_rows, differentiate, 0)
    grad_sends = []
    for k in range(1, nd):
        copy = remote(
            grads.at[own_rows], grads.at[own_rows], g_send.at[k - 1], g_recv.at[k - 1],
            {"dp": lax.rem(d + k, nd)},
        )
        copy.start()
        grad_sends.append(copy)

    depth_tile = min(256, depth)

    def pull(k):
        s = lax.rem(d + nd - k, nd)

        def step(n, _):
            at = pl.ds(pl.multiple_of(n * depth_tile, depth_tile), depth_tile)
            value = lax.dot_general(
                grads[pl.ds(pl.multiple_of(s * rows, rows), rows), :], w[at, :],
                (((1,), (1,)), ((), ())), preferred_element_type=F32,
            )
            for j in range(per):
                acc[k * per + j, :, at] = value[j * share:(j + 1) * share, :]
            return 0

        lax.fori_loop(0, depth // depth_tile, step, 0)

    def ahead(b):
        s = lax.rem(d + nd - b // per, nd)
        return s * per + b % per - v + nv

    def partner(level):
        bit = lax.rem(v // (1 << level), 2)
        return {"vocab": v + (1 - 2 * bit) * (1 << level)}

    chunk = min(16, share)

    def hop(b, level):
        return remote(sbuf.at[b], rbuf.at[level, b], r_send.at[b], r_recv.at[level, b], partner(level))

    def each_chunk(body):
        def step(i, _):
            body(pl.ds(pl.multiple_of(i * chunk, chunk), chunk))
            return 0

        lax.fori_loop(0, share // chunk, step, 0)

    def send(b, level):
        mine = lax.rem(ahead(b), 1 << level) == 0
        leaves = lax.rem(ahead(b), 2 << level) != 0

        @pl.when(jnp.logical_and(mine, leaves))
        def _():
            def body(at):
                sbuf[b, at, :] = acc[b, at, :].astype(BF16)

            each_chunk(body)
            hop(b, level).start()

    def receive(b, level):
        @pl.when(lax.rem(ahead(b), 2 << level) == 0)
        def _():
            hop(b, level).wait_recv()

            def body(at):
                acc[b, at, :] = acc[b, at, :] + rbuf[level, b, at, :].astype(F32)

            each_chunk(body)

        if level + 1 < levels:
            send(b, level + 1)

    for k in range(nd):
        if k:
            grad_sends[k - 1].wait_recv()
        pull(k)
        for j in range(per):
            send(k * per + j, 0)
        if k:
            for j in range(per):
                receive((k - 1) * per + j, 0)
    for j in range(per):
        receive((nd - 1) * per + j, 0)

    def weigh(n, _):
        at = pl.ds(pl.multiple_of(n * depth_tile, depth_tile), depth_tile)
        gwbuf[at, :] = lax.dot_general(
            spread[:, at], grads[...], (((0,), (0,)), ((), ())), preferred_element_type=F32
        ).astype(BF16)
        pltpu.make_async_copy(gwbuf.at[at], gw_ref.at[at], gw_sem.at[n]).start()
        return 0

    lax.fori_loop(0, depth // depth_tile, weigh, 0)

    for level in range(1, levels):
        for b in range(nv):
            receive(b, level)
    for b in range(nv):
        @pl.when(ahead(b) == nv)
        def _(b=b):
            def body(at):
                gh_ref[at, :] = acc[b, at, :].astype(BF16)

            each_chunk(body)

        @pl.when(ahead(b) != nv)
        def _(b=b):
            hop(b, 0).wait_send()

    for copy in hidden_sends + forwards + partial_sends + stat_sends + grad_sends:
        copy.wait_send()
    for n in range(depth // depth_tile):
        at = pl.ds(n * depth_tile, depth_tile)
        pltpu.make_async_copy(gwbuf.at[at], gw_ref.at[at], gw_sem.at[n]).wait()


def shards(nd, nv, hidden, weight, targets, cotangent):
    rows = hidden.shape[0]
    tokens = rows * nd
    depth, width = weight.shape
    share = tokens // nv
    levels = nv.bit_length() - 1
    dma = pltpu.SemaphoreType.DMA
    vmem = pl.BlockSpec(memory_space=pltpu.VMEM)
    anywhere = pl.BlockSpec(memory_space=pl.ANY)
    flops = 6 * tokens * depth * width
    loss, grad_hidden, grad_weight = pl.pallas_call(
        functools.partial(kernel, nd, nv, levels),
        out_shape=(
            jax.ShapeDtypeStruct((1, rows), F32),
            jax.ShapeDtypeStruct((share, depth), BF16),
            jax.ShapeDtypeStruct((depth, width), BF16),
        ),
        in_specs=[anywhere, anywhere, vmem, vmem],
        out_specs=(vmem, vmem, anywhere),
        scratch_shapes=[
            pltpu.VMEM((depth, width), BF16),
            pltpu.VMEM((tokens, depth), BF16),
            pltpu.VMEM((rows, width), F32),
            pltpu.VMEM((nd - 1, rows, width), WIRE),
            pltpu.VMEM((nd - 1, rows, width), WIRE),
            pltpu.VMEM((nv, 8, rows), F32),
            pltpu.VMEM((tokens, width), BF16),
            pltpu.VMEM((nv, share, depth), F32),
            pltpu.VMEM((nv, share, depth), BF16),
            pltpu.VMEM((levels, nv, share, depth), BF16),
            pltpu.VMEM((depth, width), BF16),
            pltpu.VMEM((rows, 128), jnp.int32),
            pltpu.VMEM((rows, 128), F32),
            pltpu.VMEM((rows, 128), F32),
            pltpu.VMEM((rows // 2, width), F32),
            pltpu.VMEM((nd - 1, 2, 8, rows // 2), F32),
            pltpu.VMEM((nd - 1, 2, 8, rows // 2), F32),
            pltpu.VMEM((nd - 1, rows, 128), F32),
            dma, dma, dma((depth // min(256, depth),)),
            dma((nd - 1,)), dma((nd - 1,)), dma((nd - 1,)), dma((nd - 1,)),
            dma((nd - 1, 2)), dma((nd - 1, 2)), dma((nd - 1, 2)), dma((nd - 1, 2)),
            dma((nv - 1,)), dma((nv - 1,)),
            dma((nd - 1,)), dma((nd - 1,)),
            dma((nv,)), dma((levels, nv)),
        ],
        compiler_params=pltpu.CompilerParams(
            collective_id=0, has_side_effects=True, vmem_limit_bytes=66_000_000
        ),
        cost_estimate=pl.CostEstimate(flops=flops, bytes_accessed=16 << 20, transcendentals=0),
        name="token_loss",
    )(hidden, weight, targets.reshape(1, rows), cotangent.reshape(1, rows))
    return loss.reshape(rows), grad_hidden, grad_weight


def solution(mesh):
    in_specs = (P("dp", None), P("dp", "vocab"), P("dp"), P("dp"))
    out_specs = (P("dp"), P("vocab", "dp"), P("dp", "vocab"))
    body = functools.partial(shards, mesh.shape["dp"], mesh.shape["vocab"])
    return jax.shard_map(body, mesh=mesh, in_specs=in_specs, out_specs=out_specs, check_vma=False)
```

```python
import functools

import jax
import jax.numpy as jnp
from jax import lax
from jax.experimental import pallas as pl
from jax.experimental.pallas import tpu as pltpu
from jax.sharding import PartitionSpec as P

F32 = jnp.float32
BF16 = jnp.bfloat16
WIRE = jnp.int16
STEPS = 32000.0


def kernel(
    nd, nv, levels,
    h_ref, w_hbm, t_ref, c_ref,
    loss_ref, gh_ref, gw_ref,
    w, spread, logit, psend, precv, stats, grads, acc, sbuf, rbuf, gwbuf, tcol, ccol, col,
    part_f32, usend, urecv, ucol,
    w_sem, own_sem, gw_sem,
    hs_send, hs_recv, hf_send, hf_recv, hx_send, hx_recv, p_send, p_recv, u_send, u_recv,
    st_send, st_recv, g_send, g_recv, x_send, x_recv, r_send, r_recv,
):
    d, v = lax.axis_index("dp"), lax.axis_index("vocab")
    core = lax.rem(v, 2)

    def flip(i, mask):
        for bit in range(mask.bit_length()):
            if mask >> bit & 1:
                i = i + (1 - 2 * lax.rem(i // (1 << bit), 2)) * (1 << bit)
        return i

    mate, across = flip(v, 1), flip(v, 2)
    side = lax.rem(v // 2, 2)
    depth, width = w.shape
    tokens = spread.shape[0]
    rows = tokens // nd
    half = rows // 2
    quarter = rows // 4
    share = tokens // nv
    per = rows // share

    load_w = pltpu.make_async_copy(w_hbm, w, w_sem)
    load_w.start()
    own_rows = pl.ds(pl.multiple_of(d * rows, rows), rows)
    load_own = pltpu.make_async_copy(
        h_ref.at[:, pl.ds(pl.multiple_of(d * depth, depth), depth)], spread.at[own_rows], own_sem
    )
    load_own.start()

    barrier = pltpu.get_barrier_semaphore()
    for k in range(1, nd):
        pl.semaphore_signal(barrier, inc=1, device_id={"dp": flip(d, k)})
    for k in range(1, nv):
        pl.semaphore_signal(barrier, inc=1, device_id={"vocab": lax.rem(v + k, nv)})
    pl.semaphore_wait(barrier, nd + nv - 2)

    def remote(src, dst, send, recv, where):
        return pltpu.make_async_remote_copy(
            src_ref=src, dst_ref=dst, send_sem=send, recv_sem=recv, device_id=where
        )

    def piece(s, q):
        return spread.at[pl.ds(pl.multiple_of(s * rows + q * quarter, quarter), quarter)]

    mine = 2 * side + core
    hidden_sends = []
    for k in range(1, nd):
        to = flip(d, k)
        copy = remote(
            h_ref.at[
                pl.ds(pl.multiple_of(mine * quarter, quarter), quarter),
                pl.ds(pl.multiple_of(to * depth, depth), depth),
            ],
            piece(d, mine), hs_send.at[k - 1], hs_recv.at[k - 1], {"dp": to},
        )
        copy.start()
        hidden_sends.append(copy)

    tcol[...] = jnp.broadcast_to(t_ref[...], (128, rows)).T
    ccol[...] = jnp.broadcast_to(c_ref[...], (128, rows)).T

    tile = min(256, width)
    code_rows = min(32, half)

    def project(first, count, store):
        def step(n, _):
            cols = pl.ds(pl.multiple_of(n * tile, tile), tile)
            store(cols, jnp.dot(
                spread[pl.ds(pl.multiple_of(first, count), count), :], w[:, cols],
                preferred_element_type=F32,
            ))
            return 0

        lax.fori_loop(0, width // tile, step, 0)

    load_w.wait()
    load_own.wait()

    def store_own(cols, value):
        logit[:, cols] = value

    project(d * rows, rows, store_own)

    forwards, crossings, partial_sends = [], [], []
    for turn in range(2):
        for k in range(1, nd):
            s = flip(d, k)
            part = side if turn == 0 else 1 - side
            got = piece(s, 2 * part + core)
            to_mate = remote(got, got, hf_send.at[k - 1, turn], hf_recv.at[k - 1, turn], {"vocab": mate})
            over = remote(got, got, hx_send.at[k - 1], hx_recv.at[k - 1], {"vocab": across})
            if turn == 0:
                remote(got, got, hs_send.at[k - 1], hs_recv.at[k - 1], {"dp": s}).wait_recv()
                over.start()
                crossings.append(over)
            else:
                over.wait_recv()
            to_mate.start()
            forwards.append(to_mate)
            to_mate.wait_recv()
            there = pl.ds(pl.multiple_of(part * half, half), half)

            def store_part(cols, value):
                part_f32[:, cols] = value

            project(s * rows + part * half, half, store_part)

            def encode(i, _, k=k, part=part):
                at = pl.ds(pl.multiple_of(i * code_rows, code_rows), code_rows)
                x = part_f32[at, :]
                unit = jnp.maximum(jnp.max(jnp.abs(x), axis=1, keepdims=True), 1e-30) / STEPS
                there = pl.ds(pl.multiple_of(part * half + i * code_rows, code_rows), code_rows)
                psend[k - 1, there, :] = jnp.round(x / unit).astype(jnp.int32).astype(WIRE)
                col[at, :] = jnp.broadcast_to(unit, (code_rows, 128))
                return 0

            lax.fori_loop(0, half // code_rows, encode, 0)
            usend[k - 1, turn] = col[:half, :].T[:8, :]
            for copy in (
                remote(
                    psend.at[k - 1, there], precv.at[k - 1, there],
                    p_send.at[k - 1, turn], p_recv.at[k - 1, turn], {"dp": s},
                ),
                remote(
                    usend.at[k - 1, turn], urecv.at[k - 1, turn],
                    u_send.at[k - 1, turn], u_recv.at[k - 1, turn], {"dp": s},
                ),
            ):
                copy.start()
                partial_sends.append(copy)
    for copy in partial_sends:
        copy.wait_recv()
    for k in range(1, nd):
        for turn in range(2):
            part = side if turn == 0 else 1 - side
            there = pl.ds(pl.multiple_of(part * half, half), half)
            ucol[k - 1, there, :] = jnp.broadcast_to(urecv[k - 1, turn][0:1, :], (128, half)).T

    step_rows = min(32, rows)
    column = lax.broadcasted_iota(jnp.int32, (step_rows, width), 1) + v * width
    lane = lax.broadcasted_iota(jnp.int32, (step_rows, 128), 1)

    def measure(i, _):
        at = pl.ds(pl.multiple_of(i * step_rows, step_rows), step_rows)
        x = logit[at, :]
        for k in range(1, nd):
            x = x + precv[k - 1, at, :].astype(jnp.int32).astype(F32) * ucol[k - 1, at, :1]
        top = jnp.max(x, axis=1, keepdims=True)
        e = jnp.exp(x - top)
        total = jnp.sum(e, axis=1, keepdims=True)
        pick = jnp.sum(jnp.where(column == tcol[at, :1], x, 0.0), axis=1, keepdims=True)
        logit[at, :] = e
        col[at, :] = jnp.where(lane == 0, top, jnp.where(lane == 1, total, pick))
        return 0

    lax.fori_loop(0, rows // step_rows, measure, 0)
    stats[v] = col[...].T[:8, :]
    stat_sends = []
    for k in range(1, nv):
        copy = remote(
            stats.at[v], stats.at[v], st_send.at[k - 1], st_recv.at[k - 1],
            {"vocab": lax.rem(v + k, nv)},
        )
        copy.start()
        stat_sends.append(copy)
    own_top = stats[v][0:1, :]
    for copy in stat_sends:
        copy.wait_recv()
    top = stats[0][0:1, :]
    for u in range(1, nv):
        top = jnp.maximum(top, stats[u][0:1, :])
    total = jnp.zeros_like(top)
    pick = jnp.zeros_like(top)
    for u in range(nv):
        block = stats[u]
        total = total + block[1:2, :] * jnp.exp(block[0:1, :] - top)
        pick = pick + block[2:3, :]
    loss_ref[...] = top + jnp.log(total) - pick
    scale = c_ref[...] * jnp.exp(own_top - top) / total
    col[...] = jnp.broadcast_to(scale, (128, rows)).T

    def differentiate(i, _):
        at = pl.ds(pl.multiple_of(i * step_rows, step_rows), step_rows)
        onehot = jnp.where(column == tcol[at, :1], ccol[at, :1], 0.0)
        g = logit[at, :] * col[at, :1] - onehot
        grads[pl.ds(pl.multiple_of(d * rows + i * step_rows, step_rows), step_rows), :] = g.astype(BF16)
        return 0

    lax.fori_loop(0, rows // step_rows, differentiate, 0)
    relayed = nd == 4
    grad_sends = []
    for k in range(1, nd - 1 if relayed else nd):
        copy = remote(
            grads.at[own_rows], grads.at[own_rows], g_send.at[k - 1], g_recv.at[k - 1],
            {"dp": flip(d, k)},
        )
        copy.start()
        grad_sends.append(copy)

    def relay(k):
        block = grads.at[pl.ds(pl.multiple_of(flip(d, k) * rows + (k - 1) * half, half), half)]
        return remote(block, block, x_send.at[k - 1], x_recv.at[k - 1], {"dp": flip(d, 3 - k)})

    relays = [relay(1), relay(2)] if relayed else []

    depth_tile = min(256, depth)

    def pull(k):
        s = flip(d, k)

        def step(n, _):
            at = pl.ds(pl.multiple_of(n * depth_tile, depth_tile), depth_tile)
            value = lax.dot_general(
                grads[pl.ds(pl.multiple_of(s * rows, rows), rows), :], w[at, :],
                (((1,), (1,)), ((), ())), preferred_element_type=F32,
            )
            for j in range(per):
                acc[k * per + j, :, at] = value[j * share:(j + 1) * share, :]
            return 0

        lax.fori_loop(0, depth // depth_tile, step, 0)

    def ahead(b):
        s = flip(d, b // per)
        return s * per + b % per - v + nv

    def partner(level):
        bit = lax.rem(v // (1 << level), 2)
        return {"vocab": v + (1 - 2 * bit) * (1 << level)}

    chunk = min(16, share)

    def hop(b, level):
        return remote(sbuf.at[b], rbuf.at[level, b], r_send.at[b], r_recv.at[level, b], partner(level))

    def each_chunk(body):
        def step(i, _):
            body(pl.ds(pl.multiple_of(i * chunk, chunk), chunk))
            return 0

        lax.fori_loop(0, share // chunk, step, 0)

    def send(b, level):
        mine = lax.rem(ahead(b), 1 << level) == 0
        leaves = lax.rem(ahead(b), 2 << level) != 0

        @pl.when(jnp.logical_and(mine, leaves))
        def _():
            def body(at):
                sbuf[b, at, :] = acc[b, at, :].astype(BF16)

            each_chunk(body)
            hop(b, level).start()

    def receive(b, level):
        @pl.when(lax.rem(ahead(b), 2 << level) == 0)
        def _():
            hop(b, level).wait_recv()

            def body(at):
                acc[b, at, :] = acc[b, at, :] + rbuf[level, b, at, :].astype(F32)

            each_chunk(body)

        if level + 1 < levels:
            send(b, level + 1)

    def arrive(k):
        if relayed and k == nd - 1:
            for copy in relays:
                copy.wait_recv()
        elif k:
            grad_sends[k - 1].wait_recv()
            if relayed:
                relays[k - 1].start()

    pending = []
    for k in range(nd):
        if relayed and k == 1:
            arrive(1)
            arrive(2)
        elif not (relayed and k == 2):
            arrive(k)
        pull(k)
        for j in range(per):
            send(k * per + j, 0)
        for j in range(per):
            receive(k * per + j, 0)
            pending.append(k * per + j)
        if k >= 2 and levels > 1:
            for b in pending[:per]:
                receive(b, 1)
            pending = pending[per:]

    def weigh(n, _):
        at = pl.ds(pl.multiple_of(n * depth_tile, depth_tile), depth_tile)
        gwbuf[at, :] = lax.dot_general(
            spread[:, at], grads[...], (((0,), (0,)), ((), ())), preferred_element_type=F32
        ).astype(BF16)
        pltpu.make_async_copy(gwbuf.at[at], gw_ref.at[at], gw_sem.at[n]).start()
        return 0

    lax.fori_loop(0, depth // depth_tile, weigh, 0)

    for level in range(1, levels):
        for b in pending if level == 1 else range(nv):
            receive(b, level)
    for b in range(nv):
        @pl.when(ahead(b) == nv)
        def _(b=b):
            def body(at):
                gh_ref[at, :] = acc[b, at, :].astype(BF16)

            each_chunk(body)

        @pl.when(ahead(b) != nv)
        def _(b=b):
            hop(b, 0).wait_send()

    for copy in hidden_sends + forwards + crossings + partial_sends + stat_sends + grad_sends + relays:
        copy.wait_send()
    for n in range(depth // depth_tile):
        at = pl.ds(n * depth_tile, depth_tile)
        pltpu.make_async_copy(gwbuf.at[at], gw_ref.at[at], gw_sem.at[n]).wait()


def shards(nd, nv, hidden, weight, targets, cotangent):
    rows = hidden.shape[0]
    tokens = rows * nd
    depth, width = weight.shape
    share = tokens // nv
    levels = nv.bit_length() - 1
    dma = pltpu.SemaphoreType.DMA
    vmem = pl.BlockSpec(memory_space=pltpu.VMEM)
    anywhere = pl.BlockSpec(memory_space=pl.ANY)
    flops = 6 * tokens * depth * width
    loss, grad_hidden, grad_weight = pl.pallas_call(
        functools.partial(kernel, nd, nv, levels),
        out_shape=(
            jax.ShapeDtypeStruct((1, rows), F32),
            jax.ShapeDtypeStruct((share, depth), BF16),
            jax.ShapeDtypeStruct((depth, width), BF16),
        ),
        in_specs=[anywhere, anywhere, vmem, vmem],
        out_specs=(vmem, vmem, anywhere),
        scratch_shapes=[
            pltpu.VMEM((depth, width), BF16),
            pltpu.VMEM((tokens, depth), BF16),
            pltpu.VMEM((rows, width), F32),
            pltpu.VMEM((nd - 1, rows, width), WIRE),
            pltpu.VMEM((nd - 1, rows, width), WIRE),
            pltpu.VMEM((nv, 8, rows), F32),
            pltpu.VMEM((tokens, width), BF16),
            pltpu.VMEM((nv, share, depth), F32),
            pltpu.VMEM((nv, share, depth), BF16),
            pltpu.VMEM((levels, nv, share, depth), BF16),
            pltpu.VMEM((depth, width), BF16),
            pltpu.VMEM((rows, 128), jnp.int32),
            pltpu.VMEM((rows, 128), F32),
            pltpu.VMEM((rows, 128), F32),
            pltpu.VMEM((rows // 2, width), F32),
            pltpu.VMEM((nd - 1, 2, 8, rows // 2), F32),
            pltpu.VMEM((nd - 1, 2, 8, rows // 2), F32),
            pltpu.VMEM((nd - 1, rows, 128), F32),
            dma, dma, dma((depth // min(256, depth),)),
            dma((nd - 1,)), dma((nd - 1,)), dma((nd - 1, 2)), dma((nd - 1, 2)), dma((nd - 1,)), dma((nd - 1,)),
            dma((nd - 1, 2)), dma((nd - 1, 2)), dma((nd - 1, 2)), dma((nd - 1, 2)),
            dma((nv - 1,)), dma((nv - 1,)),
            dma((nd - 1,)), dma((nd - 1,)),
            dma((2,)), dma((2,)),
            dma((nv,)), dma((levels, nv)),
        ],
        compiler_params=pltpu.CompilerParams(
            collective_id=0, has_side_effects=True, vmem_limit_bytes=66_000_000
        ),
        cost_estimate=pl.CostEstimate(flops=flops, bytes_accessed=16 << 20, transcendentals=0),
        name="token_loss",
    )(hidden, weight, targets.reshape(1, rows), cotangent.reshape(1, rows))
    return loss.reshape(rows), grad_hidden, grad_weight


def solution(mesh):
    in_specs = (P("dp", None), P("dp", "vocab"), P("dp"), P("dp"))
    out_specs = (P("dp"), P("vocab", "dp"), P("dp", "vocab"))
    body = functools.partial(shards, mesh.shape["dp"], mesh.shape["vocab"])
    return jax.shard_map(body, mesh=mesh, in_specs=in_specs, out_specs=out_specs, check_vma=False)
```
